32 devices in a mesh: dom: 32 (over z, y, x, core).
Axes of the slice: x: 2, y: 2, z: 4, core: 2. Of those that a mesh axis runs over, the one named last changes fastest.
Arguments:
- traction: float32 [16384, 3, 128], P('dom'), may hold values from -6 to 6
- fluid_coords: float32 [16384, 3, 128], P('dom'), may hold values from 0 to 1
- struct_coords: float32 [3, 32, 4096], P(None, None, 'dom'), may hold values from 0 to 1
- dest: int32 [16384, 1], P('dom'), may hold values from 0 to 31; in each aligned block of 512 rows (0 to 511, 512 to 1023, ...) at most 32 rows name the same one
- target: int32 [16384], P('dom'), may hold values from 0 to 127
- blocks: float32 [3, 96, 96, 4096], P(None, None, None, 'dom'), may hold values from -1 to 7, as said below
- columns: int32 [2, 4096], P(None, 'dom'), may hold values from 0 to 159
- halo_list: int32 [512], P('dom'), may hold values from 0 to 127
- precond: float32 [96, 96, 4096], P(None, None, 'dom'), may hold values from -1 to 1
Outputs:
- load_field: float32 [96, 4096], P(None, 'dom')
- solution: float32 [96, 4096], P(None, 'dom')
- residual: float32 [96, 4096], P(None, 'dom')
The draws below stay inside these ranges and needn't reach their ends.
Inputs may be any that keep to these rules, and one draw needn't show every extreme that they name: `dest`: among the fluid blocks of one partition no partition is named more than 32 times, a bound that some block reaches. Each diagonal block is its positive diagonal plus small full entries; coupling blocks are small full blocks.
All inputs are finite; a program needn't handle non-finite values.
Results may differ from the reference program's by a relative error of at most 0.0003.
Values sent between devices are 32-bit elements; how exact they have to be, the bound alone decides.
A program may use at most 128 MiB of HBM per device.

```python
import math
import jax
import jax.numpy as jnp
import numpy as np
from jax import lax

NODES = 128
CLUSTER = 96
SNODE = 32
FB_DEV = 512
SB_DEV = 128
HB = 16
ITERS = 2
PARTS_SIZE = 32
CAP = 32
FBLK = 16384
NBLK = 4096
HALO_ALL = 512
N_DOM = 32


def draw_blocks(key, part):
    key_jitter, key_scale = jax.random.split(jax.random.fold_in(key, 11))
    random_part = jnp.clip(jax.random.normal(key_jitter, (3, CLUSTER, CLUSTER, NBLK), jnp.float32), -3.0, 3.0)
    random_part = random_part * (0.5 / math.sqrt(3 * CLUSTER))
    scales = jnp.exp(jax.random.uniform(key_scale, (CLUSTER, NBLK), jnp.float32, math.log(2.0), math.log(6.0)))
    identity = jnp.eye(CLUSTER, dtype=jnp.float32)
    diagonal_part = identity[:, :, None] * scales[:, None, :]
    return random_part.at[0].add(diagonal_part)


def draw_precond(key, part):
    key_jitter, key_scale = jax.random.split(jax.random.fold_in(key, 13))
    random_part = jnp.clip(jax.random.normal(key_jitter, (CLUSTER, CLUSTER, NBLK), jnp.float32), -3.0, 3.0)
    random_part = random_part * (0.1 / math.sqrt(CLUSTER))
    scales = jnp.exp(jax.random.uniform(key_scale, (CLUSTER, NBLK), jnp.float32, math.log(0.15), math.log(0.5)))
    identity = jnp.eye(CLUSTER, dtype=jnp.float32)
    return random_part + identity[:, :, None] * scales[:, None, :]


def touch_ends(values, stream_key, low, high):
    place = [jax.random.randint(jax.random.fold_in(stream_key, axis), (), 0, length) for axis, length in enumerate(values.shape)]
    widest = values.shape.index(max(values.shape))
    next_to = place[:widest] + [(place[widest] + 1) % values.shape[widest]] + place[widest + 1:]
    return values.at[tuple(place)].set(low).at[tuple(next_to)].set(high)


def levels(stream_key, extent, cuts, smallest, high):
    loudness, own = 1.0, jax.random.fold_in(stream_key, 6)
    for dim, parts in cuts:
        heights = jnp.exp(jax.random.uniform(jax.random.fold_in(own, dim), (parts,), jnp.float32, smallest / len(cuts), high / len(cuts)))
        loudness = loudness * jnp.repeat(heights, extent[dim] // parts).reshape([-1 if axis == dim else 1 for axis in range(len(extent))])
    return loudness


def deal_out(key, own, number, rows, count, top, most, lean):
    sequence = jax.random.permutation(key, count)
    packed, usual = load_shares(count, rows * top, most, lean, True), load_shares(count, rows * top, most, lean, False)
    places = jnp.arange(count)

    def named(sizes, offset_by):
        used = int((sizes > 0).sum())
        fixed = max(1, used // 4)
        passed = fixed + (places - fixed + offset_by * (used - fixed)) % max(1, count - fixed)
        return jnp.zeros((count,), jnp.int32).at[sequence[jnp.where(places < fixed, places, passed)]].set(jnp.asarray(sizes, jnp.int32))

    sizes = jnp.where(number % 4 == 0, named(packed, number // 4), named(usual, number - number // 4 - 1))
    mixed = jax.random.permutation(jax.random.fold_in(own, 3), count)
    giver, receiver = mixed[0:count // 2 * 2:2], mixed[1:count // 2 * 2:2]
    slack = jnp.minimum(sizes[giver] - 1, most - sizes[receiver]) // 2
    slack = jnp.where((giver == sequence[0]) | (receiver == sequence[0]) | (sizes[receiver] == 0), 0, jnp.maximum(slack, 0))
    passed = jax.random.randint(jax.random.fold_in(own, 4), (count // 2,), 0, 1 << 20) % (slack + 1)
    sizes = sizes.at[giver].add(-passed).at[receiver].add(passed)
    members = jnp.searchsorted(jnp.cumsum(sizes), jnp.arange(rows * top), side="right").astype(jnp.int32)
    listing = members.reshape(top, rows).T
    listing = listing[jax.random.permutation(jax.random.fold_in(own, 1), rows)]
    offset_by = jax.random.randint(jax.random.fold_in(own, 2), (rows, 1), 0, top)
    return jnp.take_along_axis(listing, (jnp.arange(top)[None, :] + offset_by) % top, axis=1)


def load_shares(number_of, total, most, lean, full):
    portions = [(1 << 20) // math.isqrt(rank ** lean) + 1 for rank in range(1, number_of + 1)]
    largest = most if full else min(most, max(-(-total // number_of), total * portions[0] // sum(portions)))
    least = 1 if total - largest >= number_of - 1 else 0
    given, spare = [largest] + [least] * (number_of - 1), total - largest - least * (number_of - 1)
    while spare > 0:
        candidates = [i for i in range(1, number_of) if given[i] < largest] or [i for i in range(1, number_of) if given[i] < most]
        mass, remaining = sum([portions[i] for i in candidates]), spare
        for i in candidates:
            more = min(most - given[i], max(1, remaining * portions[i] // mass), spare)
            given[i] = given[i] + more
            spare = spare - more
    return np.array(given)


def bell_draw(own_key, extent, width, reach, pieces=(), kind=jnp.bfloat16):
    gain = levels(own_key, extent, pieces, -0.22, 0.18) if pieces else 1.0
    values = jax.random.normal(own_key, extent, jnp.float32) * width * gain
    return jnp.minimum(jnp.maximum(values, -reach), reach).astype(kind)


def setup_inputs(seed: int = 0) -> dict:
    streams_of = jax.random.split(jax.random.key(seed), 10)
    traction = bell_draw(streams_of[0], (FBLK, 3, NODES), 1.0, 6.0, ((0, 32),), jnp.float32)
    fluid_coords = jnp.clip(1.0 * jax.random.uniform(streams_of[1], (FBLK, 3, NODES), jnp.float32) ** levels(streams_of[1], (FBLK, 3, NODES), ((0, 32),), -0.2, 0.2), 0.0, 1.0)
    struct_coords = jnp.clip(1.0 * jax.random.uniform(streams_of[2], (3, SNODE, NBLK), jnp.float32) ** levels(streams_of[2], (3, SNODE, NBLK), ((2, 32),), -0.2, 0.2), 0.0, 1.0)
    dest_keys = jax.random.split(jax.random.fold_in(streams_of[3], 1), FBLK // FB_DEV)
    dest_turns = jax.random.permutation(jax.random.fold_in(streams_of[3], 3), FBLK // FB_DEV)
    dest = jax.vmap(lambda own, number: deal_out(jax.random.fold_in(streams_of[3], 2), own, number, FB_DEV, PARTS_SIZE, 1, CAP, 1))(dest_keys, dest_turns).reshape((FBLK, 1))
    target = touch_ends(jax.random.randint(streams_of[4], (FBLK,), 0, SB_DEV), jax.random.fold_in(streams_of[4], 1), 0, SB_DEV - 1).astype(jnp.int32)
    blocks = draw_blocks(jax.random.fold_in(streams_of[9], 71), 0)
    columns = touch_ends(jax.random.randint(streams_of[6], (2, NBLK), 0, SB_DEV + 2 * HB), jax.random.fold_in(streams_of[6], 1), 0, (SB_DEV + 2 * HB) - 1).astype(jnp.int32)
    halo_list = touch_ends(jax.random.randint(streams_of[7], (HALO_ALL,), 0, SB_DEV), jax.random.fold_in(streams_of[7], 1), 0, SB_DEV - 1).astype(jnp.int32)
    precond = draw_precond(jax.random.fold_in(streams_of[9], 71), 0)
    return dict(traction=traction, fluid_coords=fluid_coords, struct_coords=struct_coords, dest=dest, target=target, blocks=blocks, columns=columns, halo_list=halo_list, precond=precond)


support = 0.9

def wendland_map(fluid_pos, force, struct_pos):
    dist_sq = jnp.zeros((fluid_pos.shape[0], struct_pos.shape[2], fluid_pos.shape[2]), jnp.float32)
    for component in range(3):
        dist_sq = dist_sq + (struct_pos[:, component, :, None] - fluid_pos[:, component, None, :]) ** 2
    radius = jnp.sqrt(dist_sq) / support
    weight = jnp.maximum(1.0 - radius, 0.0) ** 4 * (4.0 * radius + 1.0)
    mapped = jnp.einsum('bjn,bcn->bcj', weight, force, precision=lax.Precision.HIGHEST)
    return mapped.reshape(mapped.shape[0], -1)

def precondition(precond, vector):
    return jnp.einsum('abi,bi->ai', precond, vector, precision=lax.Precision.HIGHEST)

def apply_operator(vector, blocks, columns, halo_list):
    per_part = jnp.transpose(vector.reshape(CLUSTER, N_DOM, SB_DEV), (1, 0, 2))
    listed = halo_list.reshape(N_DOM, HB)
    outgoing = jnp.take_along_axis(per_part, listed[:, None, :], axis=2)
    zero_rim = jnp.zeros_like(outgoing[:1])
    from_left = jnp.concatenate([zero_rim, outgoing[:-1]], axis=0)
    from_right = jnp.concatenate([outgoing[1:], zero_rim], axis=0)
    extended = jnp.concatenate([per_part, from_left, from_right], axis=2)
    result = jnp.einsum('abi,bi->ai', blocks[0], vector, precision=lax.Precision.HIGHEST)
    for neighbor in range(2):
        picks = columns[neighbor].reshape(N_DOM, 1, SB_DEV)
        taken = jnp.take_along_axis(extended, picks, axis=2)
        taken = jnp.transpose(taken, (1, 0, 2)).reshape(CLUSTER, NBLK)
        result = result + jnp.einsum('abi,bi->ai', blocks[neighbor + 1], taken, precision=lax.Precision.HIGHEST)
    return result

def reference(traction, fluid_coords, struct_coords, dest, target, blocks, columns, halo_list, precond):
    global_index = (dest[:, 0] * SB_DEV + target).astype(jnp.int32)

    def per_device(device_index):
        start = (device_index * FB_DEV).astype(jnp.int32)
        positions = lax.dynamic_slice_in_dim(fluid_coords, start, FB_DEV, 0)
        forces = lax.dynamic_slice_in_dim(traction, start, FB_DEV, 0)
        picked = lax.dynamic_slice_in_dim(global_index, start, FB_DEV, 0)
        struct_pos = jnp.transpose(jnp.take(struct_coords, picked, axis=2), (2, 0, 1))
        return wendland_map(positions, forces, struct_pos)
    mapped = lax.map(per_device, jnp.arange(N_DOM, dtype=jnp.int32)).reshape(FBLK, CLUSTER)
    load_field = jax.ops.segment_sum(mapped, global_index, num_segments=NBLK).T
    solution = jnp.zeros_like(load_field)
    residual = load_field
    shadow = load_field
    search = load_field
    alignment = jnp.sum(shadow * residual)
    for step in range(ITERS):
        search_pre = precondition(precond, search)
        image = apply_operator(search_pre, blocks, columns, halo_list)
        step_size = alignment / jnp.sum(shadow * image)
        middle = residual - step_size * image
        middle_pre = precondition(precond, middle)
        middle_image = apply_operator(middle_pre, blocks, columns, halo_list)
        smoothing = jnp.sum(middle_image * middle) / jnp.sum(middle_image * middle_image)
        solution = solution + step_size * search_pre + smoothing * middle_pre
        residual = middle - smoothing * middle_image
        new_alignment = jnp.sum(shadow * residual)
        momentum = new_alignment / alignment * (step_size / smoothing)
        search = residual + momentum * (search - smoothing * image)
        alignment = new_alignment
    return (load_field, solution, residual)
```

```python
import functools

import jax
import jax.numpy as jnp
from jax import lax
from jax.experimental import pallas as pl
from jax.experimental.pallas import tpu as pltpu
from jax.sharding import PartitionSpec as P

support = 0.9
MESH = pl.DeviceIdType.MESH
f32 = jnp.float32
bf16 = jnp.bfloat16
FIRST = 12


def iota(shape, dim):
    return lax.broadcasted_iota(jnp.int32, shape, dim)


def hot(cond):
    return jnp.where(cond, 1.0, 0.0).astype(bf16)


def dot(a, b, dims=((1,), (0,))):
    return lax.dot_general(a, b, (dims, ((), ())), preferred_element_type=f32)


def round_off(x):
    return x.astype(bf16).astype(f32)


def pieces_of(x):
    high = round_off(x)
    rest = x - high
    mid = round_off(rest)
    return high, mid, rest - mid


def split_three(x):
    return [piece.astype(bf16) for piece in pieces_of(x)]


def pick(pieces, onehot, dims):
    total = None
    for piece in pieces:
        part = dot(piece, onehot, dims)
        total = part if total is None else total + part
    return total


def planes(n):
    outer = 1
    while n % (2 * outer) == 0 and 2 * (2 * outer) ** 2 <= n:
        outer *= 2
    return outer


def window_kernel(
    parts,
    dest_hbm,
    target_hbm,
    struct_hbm,
    columns_hbm,
    halo_hbm,
    traction_hbm,
    coords_hbm,
    blocks_hbm,
    precond_hbm,
    out_ref_all,
    dest_v,
    target_v,
    columns_v,
    halo_v,
    fluid,
    blocks,
    precond,
    label_out,
    label_in,
    request_in,
    tables,
    row_v,
    row_s,
    answer_out,
    answer_in,
    mapped_out,
    mapped_in,
    stage,
    source_t,
    force_l,
    dist_a,
    dist_b,
    out_a,
    out_b,
    operand,
    taken,
    halo_out,
    halo_in,
    partial,
    small_sems,
    load_sems,
    row_sem,
    label_sems,
    request_sems,
    table_send,
    table_recv,
    answer_send,
    answer_recv,
    mapped_sems,
    halo_send,
    halo_recv,
    sum_sems,
):
    load_ref, more_load_ref, solution_ref, more_solution_ref, residual_ref, more_residual_ref = (
        out_ref_all.at[i] for i in range(6)
    )
    me = lax.axis_index("dom")
    n = parts
    outer = planes(n)
    inner = n // outer
    plane, spot = me // inner, lax.rem(me, inner)
    fluid_count = dest_v.shape[1]
    comps, snode, local = tables.shape[1:]
    nodes = coords_hbm.shape[2]
    cluster = comps * snode
    listed = halo_v.shape[1]
    cap = max(8, 2 * fluid_count // n)
    rounds = cap // 8
    per_row = local // snode
    halves = 8 // per_row
    rows = answer_in.shape[2]
    wide = per_row * local
    barrier = pltpu.get_barrier_semaphore()

    def remote(src, dst, send, recv, to):
        return pltpu.make_async_remote_copy(
            src_ref=src,
            dst_ref=dst,
            send_sem=send,
            recv_sem=recv,
            device_id=(to,),
            device_id_type=MESH,
        )

    def near(k):
        return plane * inner + lax.rem(spot + k, inner)

    def above(q):
        return lax.rem(plane + q, outer)

    for k in range(1, inner):
        pl.semaphore_signal(barrier, 1, device_id=(near(k),), device_id_type=MESH)
    for q in range(1, outer):
        pl.semaphore_signal(
            barrier, 1, device_id=(above(q) * inner + spot,), device_id_type=MESH
        )

    smalls = [
        pltpu.make_async_copy(src, dst, small_sems.at[i])
        for i, (src, dst) in enumerate(
            [
                (dest_hbm, dest_v),
                (target_hbm, target_v),
                (struct_hbm, tables.at[plane]),
                (columns_hbm, columns_v),
                (halo_hbm, halo_v),
            ]
            + [(coords_hbm.at[c], fluid.at[:, c, :]) for c in range(comps)]
            + [(traction_hbm.at[c], fluid.at[:, comps + c, :]) for c in range(comps)]
        )
    ]
    loads = [pltpu.make_async_copy(precond_hbm, precond, load_sems.at[0])]
    for which in range(3):
        loads.append(
            pltpu.make_async_copy(
                blocks_hbm.at[which], blocks.at[which], load_sems.at[which + 1]
            )
        )
    for copy in smalls + loads:
        copy.start()

    for copy in smalls[:2]:
        copy.wait()
    dest = dest_v[...]
    named = jnp.where(iota((n, fluid_count), 0) == dest, 1.0, 0.0)
    named_b = named.astype(bf16)
    earlier = hot(iota((fluid_count, fluid_count), 0) < iota((fluid_count, fluid_count), 1))
    before = jnp.sum(dot(named_b, earlier) * named, axis=0, keepdims=True)
    place = hot(iota((local, fluid_count), 0).astype(f32) == before)
    number = iota((1, fluid_count), 1)
    values = [target_v[...] + 1, number // 32, lax.rem(number, 32)]
    listing = jnp.concatenate([named * value.astype(f32) for value in values], axis=0)
    found = dot(listing.astype(bf16), place, ((1,), (1,)))
    labels = found[:n] - 1.0
    row_v[...] = (found[n : 2 * n] * 32.0 + found[2 * n :]).astype(jnp.int32)
    row_copy = pltpu.make_async_copy(row_v, row_s, row_sem.at[0])
    row_copy.start()
    for d in range(n):
        label_out[d % inner, d // inner] = labels[d : d + 1, :]
    smalls[2].wait()

    pl.semaphore_wait(barrier, inner + outer - 2)

    for k in range(1, inner):
        remote(
            label_out.at[lax.rem(spot + k, inner)],
            request_in.at[spot],
            request_sems.at[0],
            request_sems.at[1],
            near(k),
        ).start()

    def table_copy(to, slot):
        return remote(
            tables.at[plane],
            tables.at[slot],
            table_send.at[0],
            table_recv.at[slot],
            to * inner + spot,
        )

    for q in range(1, outer):
        table_copy(above(q), plane).start()
    request_in[spot] = label_out[spot]

    for copy in smalls[5:]:
        copy.wait()
    row_copy.wait()

    kappa = 4.0 / support
    middle = 0.5
    ones8 = jnp.ones((8, nodes), f32)
    zeros8 = jnp.zeros((8, nodes), f32)

    def receiver(t):
        p = lax.rem(spot + inner - lax.rem(t, inner), inner)
        return above(t // inner + 1) * inner + p

    def prepare(t):
        d = receiver(t)
        for s in range(cap):
            row = jnp.clip(row_s[d, s], 0, fluid_count - 1)
            stage[s * 8 : s * 8 + 8, :] = fluid[row]
        for q in range(rounds):
            def get(c):
                return stage[pl.ds(q * 64 + c, 8, stride=8), :]

            pos = [(get(c) - middle) * kappa for c in range(comps)]
            square = pos[0] * pos[0] + pos[1] * pos[1] + pos[2] * pos[2]
            twice = [p * -2.0 for p in pos]
            fh = [round_off(p) for p in twice]
            fm = [p - h for p, h in zip(twice, fh)]
            stack = fh + fm + fh + [ones8] * 3 + list(pieces_of(square))
            stack = stack + [zeros8] * (nodes // 8 - len(stack))
            block = jnp.concatenate(stack, axis=0)
            source_t[t, q] = jnp.transpose(block).astype(bf16)
            force = jnp.concatenate([get(comps + c) * (1.0 / 256.0) for c in range(comps)], axis=0)
            high = round_off(force)
            rest = force - high
            left = jnp.concatenate([high, rest], axis=0).astype(bf16)
            right = jnp.concatenate([high, jnp.zeros_like(high)], axis=0).astype(bf16)
            force_l[t, q, :, :nodes] = left
            force_l[t, q, :, nodes:] = right

    first = FIRST * n // 32

    @pl.loop(0, first)
    def _(t):
        prepare(t)

    def wait_all(out_ref, in_ref, send_sem, recv_sem, count):
        span = pl.ds(0, count)
        return remote(out_ref.at[span], in_ref.at[span], send_sem, recv_sem, near(1))

    wait_all(label_out, request_in, request_sems.at[0], request_sems.at[1], inner - 1).wait()

    seg = iota((1, local), 1) // snode
    source_rows = inner * rows
    repeat = hot(iota((source_rows, inner), 0) // rows == iota((source_rows, inner), 1))
    own_slot = iota((source_rows, local), 1) // per_row == lax.rem(
        iota((source_rows, local), 0), rows
    )
    lane_of = iota((source_rows, local), 1).astype(f32)
    fans = [hot(lax.rem(iota((local, local), 0), per_row) == s) for s in range(per_row)]

    def answer_copy(z, p, slot, to):
        return remote(
            answer_out.at[z, p],
            answer_in.at[slot],
            answer_send.at[0],
            answer_recv.at[slot],
            to,
        )

    @pl.loop(1, outer + 1)
    def _(q):
        z = above(q)

        @pl.when(q < outer)
        def _():
            table_copy(z, z).wait_recv()

        asked = jnp.concatenate([request_in[s, z] for s in range(inner)], axis=0).astype(bf16)
        spread = jnp.where(own_slot, dot(repeat, asked), 0.0).astype(bf16)
        picks = jnp.concatenate([hot(dot(spread, fan) == lane_of) for fan in fans], axis=0)
        table = tables[z]
        tiled = [
            jnp.concatenate([piece[c] for c in range(comps) for _ in range(per_row)], axis=0)
            for piece in split_three(table)
        ]
        found = None
        for piece in tiled:
            part = dot(picks, piece, ((1,), (1,)))
            found = part if found is None else found + part
        for c in range(comps):
            total = None
            for s in range(per_row):
                part = found[s * source_rows : (s + 1) * source_rows, c * local : (c + 1) * local]
                total = part if total is None else jnp.where(seg == s, part, total)
            for s in range(inner):
                answer_out[z, s, c] = total[s * rows : (s + 1) * rows]

        @pl.loop(1, inner)
        def _(k):
            answer_copy(z, lax.rem(spot + k, inner), z * inner + spot, near(k)).start()

        answer_in[z * inner + spot] = answer_out[z, spot]

    def label_copy(to, slot):
        return remote(
            label_out.at[lax.rem(to, inner), to // inner],
            label_in.at[slot],
            label_sems.at[0],
            label_sems.at[1],
            to,
        )

    @pl.loop(1, n)
    def _(k):
        label_copy(lax.rem(me + k, n), me).start()

    label_in[me] = label_out[spot, plane]

    @pl.loop(first, n)
    def _(t):
        prepare(t)

    masks = [
        iota((8, local), 0) == h * per_row + iota((8, local), 1) // snode for h in range(halves)
    ]
    mask_ones = jnp.concatenate([jnp.where(mask, 1.0, 0.0) for mask in masks], axis=1)
    group = 8
    sub = iota((group, local), 0)

    def gather_rows(sums):
        shift = 1
        while len(sums) > 1:
            keep = lax.rem(sub // shift, 2) == 0
            sums = [
                jnp.where(keep, x, y) + pltpu.roll(jnp.where(keep, y, x), group - shift, 0)
                for x, y in zip(sums[0::2], sums[1::2])
            ]
            shift *= 2
        return sums[0]

    def mapped_copy(to, slot):
        return remote(
            mapped_out.at[to], mapped_in.at[slot], mapped_sems.at[0], mapped_sems.at[1], to
        )

    def approach(t, d, dist_ref):
        pos = [(answer_in[d, c] - middle) * kappa for c in range(comps)]
        square = pos[0] * pos[0] + pos[1] * pos[1] + pos[2] * pos[2]
        high_s = [round_off(p) for p in pos]
        rest_s = [p - h for p, h in zip(pos, high_s)]
        square_s = pieces_of(square)
        for q in range(rounds):
            def widen(piece):
                whole = [
                    jnp.where(
                        masks[h],
                        jnp.broadcast_to(
                            piece[q * halves + h : q * halves + h + 1, :], (8, local)
                        ),
                        0.0,
                    )
                    for h in range(halves)
                ]
                return jnp.concatenate(whole, axis=1)

            sh = [widen(piece) for piece in high_s]
            sm = [widen(piece) for piece in rest_s]
            sq = [widen(piece) for piece in square_s]
            stack = sh + sh + sm + sq + [mask_ones] * 3
            stack = stack + [jnp.zeros_like(mask_ones)] * (nodes // 8 - len(stack))
            close = jnp.concatenate(stack, axis=0).astype(bf16)
            dist_ref[q] = dot(source_t[t, q], close)

    def weigh(t, dist_ref, out_ref):
        for q in range(rounds):
            highs, lows = [], []
            for r in range(0, nodes, 16):
                dist = jnp.maximum(dist_ref[q, r : r + 16, :], 1e-30)
                u = jnp.maximum(4.0 - dist * lax.rsqrt(dist), 0.0)
                u2 = u * u
                phi = u2 * u2 * (5.0 - u)
                high = phi.astype(bf16)
                highs.append(high)
                lows.append((phi - high.astype(f32)).astype(bf16))
            out_ref[q] = dot(force_l[t, q], jnp.concatenate(highs + lows, axis=0))

    def collect(d, out_ref):
        lines = [[] for _ in range(comps)]
        for q in range(rounds):
            for c in range(comps):
                out = out_ref[q, 8 * c : 8 * c + 8, :] + out_ref[
                    q, 8 * (comps + c) : 8 * (comps + c) + 8, :
                ]
                for h in range(halves):
                    lines[c].append(jnp.where(masks[h], out[:, h * local : (h + 1) * local], 0.0))
        for c in range(comps):
            full = lines[c] + [jnp.zeros((8, local), f32)] * (-len(lines[c]) % group)
            for r in range(0, len(full), group):
                mapped_out[d, c, r : r + group, :] = gather_rows(full[r : r + group])

    def meet(t):
        d = receiver(t)

        @pl.when(jnp.logical_and(lax.rem(t, inner) != 0, t < n))
        def _():
            answer_copy(plane, spot, d, d).wait_recv()

    def hand_over(t):
        d = receiver(t)

        @pl.when(jnp.logical_and(t >= 0, d != me))
        def _():
            mapped_copy(d, me).start()

    approach(0, receiver(0), dist_a)

    @pl.loop(0, n // 2)
    def _(i):
        t = 2 * i
        meet(t + 1)
        weigh(t, dist_a, out_a)
        approach(t + 1, receiver(t + 1), dist_b)
        before = jnp.maximum(t - 1, 0)
        collect(receiver(before), out_b)
        hand_over(t - 1)
        following = jnp.minimum(t + 2, n - 1)
        meet(t + 2)
        weigh(t + 1, dist_b, out_b)
        approach(following, receiver(following), dist_a)
        collect(receiver(t), out_a)
        hand_over(t)

    collect(receiver(n - 1), out_b)
    hand_over(n - 1)
    mapped_in[me] = mapped_out[me]

    columns = columns_v
    for copy in smalls[3:5]:
        copy.wait()
    rows_i = iota((local, local), 0)
    rim = iota((listed, local), 0)
    cols = columns[...]
    own_hot = jnp.concatenate([hot(rows_i == cols[k : k + 1, :]) for k in range(2)], axis=1)
    left_hot = jnp.concatenate([hot(rim + local == cols[k : k + 1, :]) for k in range(2)], axis=1)
    right_hot = jnp.concatenate(
        [hot(rim + (local + listed) == cols[k : k + 1, :]) for k in range(2)], axis=1
    )
    send_cols = hot(iota((local, listed), 0) == halo_v[...])
    eye = hot(iota((listed, listed), 0) == iota((listed, listed), 1))
    send_hot = dot(eye, send_cols, ((1,), (1,))).astype(bf16)

    wait_all(label_in, label_in, label_sems.at[0], label_sems.at[1], n - 1).wait()
    asked = jnp.concatenate([label_in[s] for s in range(n)], axis=0).astype(bf16)
    total_rows = n * rows
    repeat = hot(iota((total_rows, n), 0) // rows == iota((total_rows, n), 1))
    spread = dot(repeat, asked)
    spread = jnp.where(
        iota((total_rows, local), 1) // per_row == lax.rem(iota((total_rows, local), 0), rows),
        spread,
        0.0,
    ).astype(bf16)
    fan = hot(lax.rem(iota((local, wide), 0), per_row) == iota((local, wide), 1) // local)
    wanted = dot(spread, fan)
    onehot = hot(wanted == lax.rem(iota((total_rows, wide), 1), local).astype(f32))

    for z in range(1, outer):
        table_copy(above(z), above(z)).wait_send()
    wait_all(answer_in, answer_in, answer_send.at[0], answer_recv.at[0], outer * (inner - 1)).wait_send()
    wait_all(mapped_out, mapped_in, mapped_sems.at[0], mapped_sems.at[1], n - 1).wait()

    for c in range(comps):
        came = jnp.concatenate([mapped_in[s, c] for s in range(n)], axis=0)
        turned = jnp.transpose(came)
        full = pick(split_three(turned), onehot, ((1,), (0,)))
        total = None
        for s in range(per_row):
            part = full[s * snode : (s + 1) * snode, s * local : (s + 1) * local]
            total = part if total is None else total + part
        load_ref[c * snode : (c + 1) * snode, :] = total

    def multiply(matrices, vectors, out_ref):
        @pl.loop(0, cluster // group)
        def _(g):
            start = pl.multiple_of(g * group, group)
            sums = [None] * group
            for tile in range(cluster // group):
                span = slice(tile * group, (tile + 1) * group)
                for matrix, vector in zip(matrices, vectors):
                    piece = vector[span, :]
                    for row in range(group):
                        term = matrix[start + row, span, :] * piece
                        sums[row] = term if sums[row] is None else sums[row] + term
            out_ref[pl.ds(start, group), :] = gather_rows(sums)

    def halo_copy(step, side):
        peer = me + 1 if side == 0 else me - 1
        return pltpu.make_async_remote_copy(
            src_ref=halo_out.at[step],
            dst_ref=halo_in.at[step, side],
            send_sem=halo_send.at[step, side],
            recv_sem=halo_recv.at[step, side],
            device_id=(peer,),
            device_id_type=MESH,
        )

    def apply(step, vector):
        operand[0] = vector
        if step == 0:
            loads[0].wait()
        multiply([precond], [operand.at[0]], operand.at[1])
        pre = operand[1]
        pieces = split_three(pre)
        outgoing = None
        for piece in pieces:
            part = dot(send_hot, piece, ((1,), (1,)))
            outgoing = part if outgoing is None else outgoing + part
        halo_out[step] = outgoing

        @pl.when(me < n - 1)
        def _():
            halo_copy(step, 0).start()

        @pl.when(me > 0)
        def _():
            halo_copy(step, 1).start()

        near = pick(pieces, own_hot, ((1,), (0,)))
        if step == 0:
            for copy in loads[1:]:
                copy.wait()
        multiply([blocks.at[0]], [operand.at[1]], operand.at[3])

        @pl.when(me < n - 1)
        def _():
            halo_copy(step, 0).wait_send()
            halo_copy(step, 1).wait_recv()

        @pl.when(me > 0)
        def _():
            halo_copy(step, 1).wait_send()
            halo_copy(step, 0).wait_recv()

        left = jnp.where(me > 0, halo_in[step, 0], 0.0)
        right = jnp.where(me < n - 1, halo_in[step, 1], 0.0)
        near = near + pick(split_three(left), left_hot, ((0,), (0,)))
        near = near + pick(split_three(right), right_hot, ((0,), (0,)))
        taken[0] = near[:, :local]
        taken[1] = near[:, local:]
        multiply([blocks.at[1], blocks.at[2]], [taken.at[0], taken.at[1]], operand.at[2])
        return pre, operand[2] + operand[3]

    lanes = iota((1, local), 1)

    def sum_copy(turn, source, to):
        return pltpu.make_async_remote_copy(
            src_ref=partial.at[turn, source],
            dst_ref=partial.at[turn, source],
            send_sem=sum_sems.at[turn, 0],
            recv_sem=sum_sems.at[turn, 1],
            device_id=(to,),
            device_id_type=MESH,
        )

    def send_sums(turn, pairs):
        packed = jnp.zeros((1, local), f32)
        for index, (x, y) in enumerate(pairs):
            value = jnp.sum(jnp.sum(x * y, axis=0, keepdims=True), axis=1, keepdims=True)
            packed = jnp.where(lanes == index, value, packed)
        partial[turn, me] = packed

        @pl.loop(1, n)
        def _(k):
            sum_copy(turn, me, lax.rem(me + k, n)).start()

    def take_sums(turn, count):
        wait_all(
            partial.at[turn], partial.at[turn], sum_sems.at[turn, 0], sum_sems.at[turn, 1], n - 1
        ).wait()
        total = jnp.sum(partial[turn], axis=0)
        return [
            jnp.sum(jnp.where(lanes == index, total, 0.0), axis=1, keepdims=True)
            for index in range(count)
        ]

    v0 = load_ref[...]
    z0, v1 = apply(0, v0)
    z1, v2 = apply(1, v1)
    send_sums(0, [(v0, v0), (v0, v1), (v0, v2), (v1, v1), (v1, v2), (v2, v2)])
    z2, v3 = apply(2, v2)
    g00, g01, g02, g11, g12, g22 = take_sums(0, 6)
    step_size = g00 / g01
    crossed = g01 - step_size * (g02 + g11) + step_size * step_size * g12
    squared = g11 - 2.0 * step_size * g12 + step_size * step_size * g22
    smoothing = crossed / squared
    solution = step_size * z0 + smoothing * (z0 - step_size * z1)
    residual = (v0 - step_size * v1) - smoothing * (v1 - step_size * v2)
    alignment = (g00 - step_size * g01) - smoothing * (g01 - step_size * g02)
    momentum = (alignment / g00) * (step_size / smoothing)
    pre = (z0 - step_size * z1) - smoothing * (z1 - step_size * z2)
    q = (v1 - step_size * v2) - smoothing * (v2 - step_size * v3)
    p0 = pre + momentum * (z0 - smoothing * z1)
    image = q + momentum * (v1 - smoothing * v2)
    p1, y = apply(3, image)
    send_sums(
        1,
        [
            (v0, residual),
            (v0, image),
            (q, residual),
            (q, image),
            (y, residual),
            (y, image),
            (q, q),
            (q, y),
            (y, y),
        ],
    )
    sr, si, qr, qi, yr, yi, qq, qy, yy = take_sums(1, 9)
    step_size = sr / si
    crossed = qr - step_size * (qi + yr) + step_size * step_size * yi
    squared = qq - 2.0 * step_size * qy + step_size * step_size * yy
    smoothing = crossed / squared
    solution_ref[...] = solution + step_size * p0
    more_solution_ref[...] = smoothing * (pre - step_size * p1)
    residual_ref[...] = residual - step_size * image
    more_residual_ref[...] = smoothing * (q - step_size * y)
    more_load_ref[...] = jnp.zeros_like(v0)


def on_device(
    traction, fluid_coords, struct_coords, dest, target, blocks, columns, halo_list, precond
):
    n = lax.axis_size("dom")
    outer = planes(n)
    inner = n // outer
    fluid_count, comps, nodes = traction.shape
    cluster = blocks.shape[1]
    snode, local = struct_coords.shape[1:]
    listed = halo_list.shape[0]
    cap = max(8, 2 * fluid_count // n)
    rounds = cap // 8
    rows = max(8, cap // (local // snode))
    vmem = pl.BlockSpec(memory_space=pltpu.VMEM)
    hbm = pl.BlockSpec(memory_space=pl.ANY)
    field = jax.ShapeDtypeStruct((6, cluster, local), f32)
    exchange = pltpu.VMEM((n, comps, rows, local), f32)
    dma = pltpu.SemaphoreType.DMA
    out = pl.pallas_call(
        functools.partial(window_kernel, n),
        out_shape=field,
        in_specs=[hbm] * 9,
        out_specs=vmem,
        scratch_shapes=[
            pltpu.VMEM((1, fluid_count), jnp.int32),
            pltpu.VMEM((1, fluid_count), jnp.int32),
            pltpu.VMEM(columns.shape, jnp.int32),
            pltpu.VMEM((1, listed), jnp.int32),
            pltpu.VMEM((fluid_count, 8, nodes), f32),
            pltpu.VMEM(blocks.shape, f32),
            pltpu.VMEM(precond.shape, f32),
            pltpu.VMEM((inner, outer, 1, local), f32),
            pltpu.VMEM((n, 1, local), f32),
            pltpu.VMEM((inner, outer, 1, local), f32),
            pltpu.VMEM((outer,) + struct_coords.shape, f32),
            pltpu.VMEM((n, local), jnp.int32),
            pltpu.SMEM((n, local), jnp.int32),
            pltpu.VMEM((outer, inner, comps, rows, local), f32),
            exchange,
            exchange,
            exchange,
            pltpu.VMEM((8 * cap + 64, nodes), f32),
            pltpu.VMEM((n, rounds, nodes, nodes), bf16),
            pltpu.VMEM((n, rounds, 16 * comps, 2 * nodes), bf16),
            pltpu.VMEM((rounds, nodes, 2 * nodes), f32),
            pltpu.VMEM((rounds, nodes, 2 * nodes), f32),
            pltpu.VMEM((rounds, 16 * comps, 2 * nodes), f32),
            pltpu.VMEM((rounds, 16 * comps, 2 * nodes), f32),
            pltpu.VMEM((4, cluster, local), f32),
            pltpu.VMEM((2, cluster, local), f32),
            pltpu.VMEM((4, listed, cluster), f32),
            pltpu.VMEM((4, 2, listed, cluster), f32),
            pltpu.VMEM((2, n, 1, local), f32),
            dma((5 + 2 * comps,)),
            dma((4,)),
            dma((1,)),
            dma((2,)),
            dma((2,)),
            dma((1,)),
            dma((outer,)),
            dma((1,)),
            dma((n,)),
            dma((2,)),
            dma((4, 2)),
            dma((4, 2)),
            dma((2, 2)),
        ],
        compiler_params=pltpu.CompilerParams(collective_id=0, has_side_effects=True),
        name="window",
    )(
        dest.reshape(1, fluid_count),
        target.reshape(1, fluid_count),
        struct_coords,
        columns,
        halo_list.reshape(1, listed),
        jnp.transpose(traction, (1, 0, 2)),
        jnp.transpose(fluid_coords, (1, 0, 2)),
        blocks,
        precond,
    )
    return (out[0] + out[1], out[2] + out[3], out[4] - out[5])


def solution(mesh):
    return jax.shard_map(
        on_device,
        mesh=mesh,
        in_specs=(
            P("dom", None, None),
            P("dom", None, None),
            P(None, None, "dom"),
            P("dom", None),
            P("dom"),
            P(None, None, None, "dom"),
            P(None, "dom"),
            P("dom"),
            P(None, None, "dom"),
        ),
        out_specs=(P(None, "dom"), P(None, "dom"), P(None, "dom")),
        check_vma=False,
    )
```
